32 devices in a mesh: gx: 4 (over x, core), gy: 8 (over z, y).
Axes of the slice: x: 2, y: 2, z: 4, core: 2. Of those that a mesh axis runs over, the one named last changes fastest.
Arguments:
- fields: float32 [5, 32, 32, 1024], P(None, None, 'gx', 'gy'), may hold values from -20 to 20, as said below
- coriolis: float32 [32], P('gx'), may hold values from 0.5 to 1.5
- slope_east: float32 [32, 1024], P('gx', 'gy'), may hold values from -3 to 3
- slope_north: float32 [32, 1024], P('gx', 'gy'), may hold values from -3 to 3
Outputs:
- updated: float32 [4, 32, 32, 1024], P(None, None, 'gx', 'gy')
The draws below stay inside these ranges and needn't reach their ends.
Inputs may be any that keep to these rules, and one draw needn't show every extreme that they name: `fields`: components in order: velocity along x, velocity along y, vertical velocity, potential temperature, pressure perturbation.
All inputs are finite; a program needn't handle non-finite values.
Results may differ from the reference program's by a relative error of at most 0.0003.
Values sent between devices are 32-bit elements; how exact they have to be, the bound alone decides.
A program may use at most 64 MiB of HBM per device.

```python
import jax
import jax.numpy as jnp
from jax import lax

NZ = 32
CY = 8
NX = 1024
NY = 32
N_GX = 4


def draw_fields(key, part):
    noise_key, amp_key = jax.random.split(key, 2)
    shape = (5, NZ, NY, NX)
    across = jnp.arange(NX, dtype=jnp.float32) / NX
    along = jnp.arange(NY, dtype=jnp.float32) / NY
    noise = jnp.clip(jax.random.normal(noise_key, shape, jnp.float32), -6.0, 6.0)
    ramp = 1.0 + along[:, None] + across[None, :]
    amplitude = jax.random.uniform(amp_key, (NZ,), jnp.float32, 0.5, 2.0)
    theta = noise[3] + amplitude[:, None, None] * ramp[None]
    return jnp.concatenate([noise[:3], theta[None], noise[4:]], axis=0)


def level_of(own_key, extent, shards, low, largest):
    level = 1.0
    for dim, blocks in shards:
        steps = jax.random.uniform(jax.random.fold_in(jax.random.fold_in(own_key, 6), dim), (blocks,), jnp.float32, low / len(shards), largest / len(shards))
        level = level * jnp.repeat(jnp.exp(steps), extent[dim] // blocks).reshape((-1,) + (1,) * (len(extent) - 1 - dim))
    return level


def gaussian(own_key, shape, scale, reach, cuts=(), kind=jnp.bfloat16):
    loudness = level_of(own_key, shape, cuts, -0.22, 0.18) if cuts else 1.0
    values = jax.random.normal(own_key, shape, jnp.float32) * scale * loudness
    return jnp.minimum(jnp.maximum(values, -reach), reach).astype(kind)


def setup_inputs(seed: int = 0) -> dict:
    keys = jax.random.split(jax.random.key(seed), 5)
    fields = draw_fields(jax.random.fold_in(keys[4], 71), 0)
    coriolis = jnp.clip(0.5 + 1.0 * jax.random.uniform(keys[1], (NY,), jnp.float32) ** level_of(keys[1], (NY,), ((0, 4),), -0.2, 0.2), 0.5, 1.5)
    slope_east = gaussian(keys[2], (NY, NX), 0.5, 3.0, ((0, 4), (1, 8)), jnp.float32)
    slope_north = gaussian(keys[3], (NY, NX), 0.5, 3.0, ((0, 4), (1, 8)), jnp.float32)
    return dict(fields=fields, coriolis=coriolis, slope_east=slope_east, slope_north=slope_north)


WENO_EPS = 1e-06
SECTION_DT = 0.3
SMAG_COEF = 0.06
BACKGROUND = 0.05
BUOYANCY = 0.5

def window(array, start, length, axis):
    return lax.slice_in_dim(array, start, start + length, axis=axis)

def weno_face(outer_low, inner_low, middle, inner_high, outer_high):
    smooth_zero = 13.0 / 12.0 * (outer_low - 2.0 * inner_low + middle) ** 2 + 0.25 * (outer_low - 4.0 * inner_low + 3.0 * middle) ** 2
    smooth_one = 13.0 / 12.0 * (inner_low - 2.0 * middle + inner_high) ** 2 + 0.25 * (inner_low - inner_high) ** 2
    smooth_two = 13.0 / 12.0 * (middle - 2.0 * inner_high + outer_high) ** 2 + 0.25 * (3.0 * middle - 4.0 * inner_high + outer_high) ** 2
    guess_zero = (2.0 * outer_low - 7.0 * inner_low + 11.0 * middle) / 6.0
    guess_one = (-inner_low + 5.0 * middle + 2.0 * inner_high) / 6.0
    guess_two = (2.0 * middle + 5.0 * inner_high - outer_high) / 6.0
    weight_zero = 0.1 / (WENO_EPS + smooth_zero) ** 2
    weight_one = 0.6 / (WENO_EPS + smooth_one) ** 2
    weight_two = 0.3 / (WENO_EPS + smooth_two) ** 2
    total = weight_zero + weight_one + weight_two
    return (weight_zero * guess_zero + weight_one * guess_one + weight_two * guess_two) / total

def faces_along(values, speed, axis, count):
    parts = [window(values, offset, count + 1, axis) for offset in range(6)]
    low_side = weno_face(parts[0], parts[1], parts[2], parts[3], parts[4])
    high_side = weno_face(parts[5], parts[4], parts[3], parts[2], parts[1])
    face_speed = (window(speed, 2, count + 1, axis) + window(speed, 3, count + 1, axis)) * 0.5
    return jnp.maximum(face_speed, 0.0) * low_side + jnp.minimum(face_speed, 0.0) * high_side

def divergence(flux, axis, count):
    return window(flux, 1, count, axis) - window(flux, 0, count, axis)

def section_update(extended, pressure, coriolis, slope_east, slope_north, theta_mean):
    depth = extended.shape[1]
    rows = extended.shape[2] - 6
    cols = extended.shape[3] - 6
    centre = extended[:, :, 3:-3, 3:-3]
    along_x = extended[:, :, 3:-3, :]
    flux_x = faces_along(along_x, along_x[0:1], 3, cols)
    along_y = extended[:, :, :, 3:-3]
    flux_y = faces_along(along_y, along_y[1:2], 2, rows)
    padded_z = jnp.pad(centre, ((0, 0), (3, 3), (0, 0), (0, 0)), mode='edge')
    flux_z = faces_along(padded_z, padded_z[2:3], 1, depth)
    face_index = lax.broadcasted_iota(jnp.int32, (1, depth + 1, 1, 1), 1)
    inside = jnp.logical_and(face_index > 0, face_index < depth).astype(flux_z.dtype)
    flux_z = flux_z * inside
    advection = -(divergence(flux_x, 3, cols) + divergence(flux_y, 2, rows) + divergence(flux_z, 1, depth))
    speed_x = extended[0]
    speed_y = extended[1]
    strain_xx = (speed_x[:, 2:-2, 3:-1] - speed_x[:, 2:-2, 1:-3]) * 0.5
    strain_yy = (speed_y[:, 3:-1, 2:-2] - speed_y[:, 1:-3, 2:-2]) * 0.5
    shear = (speed_x[:, 3:-1, 2:-2] - speed_x[:, 1:-3, 2:-2]) * 0.5 + (speed_y[:, 2:-2, 3:-1] - speed_y[:, 2:-2, 1:-3]) * 0.5
    eddy = SMAG_COEF * jnp.sqrt(2.0 * (strain_xx * strain_xx + strain_yy * strain_yy) + shear * shear + BACKGROUND)
    border = extended[:, :, 2:-2, 2:-2]
    eddy_x = (eddy[:, 1:-1, 1:] + eddy[:, 1:-1, :-1]) * 0.5
    diffuse_x = eddy_x * (border[:, :, 1:-1, 1:] - border[:, :, 1:-1, :-1])
    eddy_y = (eddy[:, 1:, 1:-1] + eddy[:, :-1, 1:-1]) * 0.5
    diffuse_y = eddy_y * (border[:, :, 1:, 1:-1] - border[:, :, :-1, 1:-1])
    mixing = diffuse_x[:, :, :, 1:] - diffuse_x[:, :, :, :-1] + diffuse_y[:, :, 1:, :] - diffuse_y[:, :, :-1, :]
    press_x = (pressure[:, 1:-1, 2:] - pressure[:, 1:-1, :-2]) * 0.5
    press_y = (pressure[:, 2:, 1:-1] - pressure[:, :-2, 1:-1]) * 0.5
    column = jnp.pad(pressure[:, 1:-1, 1:-1], ((1, 1), (0, 0), (0, 0)), mode='edge')
    press_z = (column[2:] - column[:-2]) * 0.5
    level_index = lax.broadcasted_iota(jnp.int32, (depth, 1, 1), 0).astype(centre.dtype)
    level_factor = 1.0 - (level_index + 0.5) / depth
    turning = coriolis[None, :, None]
    force_u = -(press_x - slope_east[None] * level_factor * press_z) + turning * centre[1]
    force_v = -(press_y - slope_north[None] * level_factor * press_z) - turning * centre[0]
    force_w = -press_z + BUOYANCY * (centre[3] - theta_mean[:, None, None])
    forcing = jnp.stack([force_u, force_v, force_w, jnp.zeros_like(force_w)])
    return centre + SECTION_DT * (advection + mixing + forcing)

def reference(fields, coriolis, slope_east, slope_north):
    theta_mean = lax.optimization_barrier(jnp.sum(fields[3], axis=(1, 2))) / (NX * NY)
    padded = jnp.pad(fields, ((0, 0), (0, 0), (3, 3), (3, 3)))

    def one_block(block):
        start = (block * CY).astype(jnp.int32)
        piece = lax.dynamic_slice_in_dim(padded, start, CY + 6, 2)
        turning = lax.dynamic_slice_in_dim(coriolis, start, CY, 0)
        east = lax.dynamic_slice_in_dim(slope_east, start, CY, 0)
        north = lax.dynamic_slice_in_dim(slope_north, start, CY, 0)
        return section_update(piece[:4], piece[4, :, 2:-2, 2:-2], turning, east, north, theta_mean)
    blocks = lax.map(one_block, jnp.arange(N_GX, dtype=jnp.int32))
    return jnp.transpose(blocks, (1, 2, 0, 3, 4)).reshape(4, NZ, NY, NX)
```

```python
import functools

import jax
import jax.numpy as jnp
from jax import lax
from jax.experimental import pallas as pl
from jax.experimental.pallas import tpu as pltpu
from jax.sharding import PartitionSpec as P

WENO_EPS = 1e-06
SECTION_DT = 0.3
SMAG_COEF = 0.06
BACKGROUND = 0.05
BUOYANCY = 0.5
MESH = pl.DeviceIdType.MESH
HALF_DT = 0.5 * SECTION_DT
LANES = 128
ROWS = 8


def weno_flux(cells, positive, speed, weight):
    q0, q1, q2, q3, q4, q5 = cells
    d0, d1, d2, d3, d4 = q1 - q0, q2 - q1, q3 - q2, q4 - q3, q5 - q4
    e1 = jnp.where(positive, d0, d4)
    e2 = jnp.where(positive, d1, d3)
    e3 = d2
    e4 = jnp.where(positive, d3, d1)
    centre = jnp.where(positive, q2, q3)
    sa, sb, sc = e2 - e1, e3 - e2, e4 - e3
    eps = 4.0 * WENO_EPS
    k = 13.0 / 3.0
    x0 = 3.0 * e2 - e1
    x1 = e2 + e3
    x2 = 3.0 * e3 - e4
    y0 = (k * sa) * sa + (x0 * x0 + eps)
    y1 = (k * sb) * sb + (x1 * x1 + eps)
    y2 = (k * sc) * sc + (x2 * x2 + eps)
    m0, m1, m2 = y1 * y2, y0 * y2, y0 * y1
    w0 = m0 * m0
    w1 = 6.0 * (m1 * m1)
    w2 = 3.0 * (m2 * m2)
    bottom = w0 + w1 + w2
    first = w0 * (sb - sa)
    top = first + first + w2 * (sc - sb)
    return speed * centre + weight * ((x1 + e3) - top / bottom)


def kernel(n_gx, n_gy, depth, fields, coriolis, east, north, out,
           A, acc, dm, dp, dux, dvx, EA, SX, RX, YH, DR, DP, T0, T1, R1, R2,
           in_sem, y_send, y_recv, x_send, x_recv, d_send, d_recv, t_send, t_recv, s_send, s_recv):
    gx = lax.axis_index("gx")
    gy = lax.axis_index("gy")
    tiles = depth // ROWS
    diag = [(1, 1), (1, -1), (-1, 1), (-1, -1)]

    def exists(dx, dy):
        cond = None
        for pos, d, n in ((gx, dx, n_gx), (gy, dy, n_gy)):
            if d == 0:
                continue
            c = (pos + d < n) if d > 0 else (pos + d >= 0)
            cond = c if cond is None else jnp.logical_and(cond, c)
        return cond

    def target(dx, dy):
        return {"gx": gx + dx, "gy": gy + dy}

    loads = []
    for q in (3, 0, 1, 2, 4):
        c = pltpu.make_async_copy(fields.at[q], A.at[q], in_sem.at[q])
        c.start()
        loads.append(c)

    barrier = pltpu.get_barrier_semaphore()
    for k in range(1, n_gx):
        pl.semaphore_signal(barrier, inc=1, device_id={"gx": lax.rem(gx + k, n_gx)}, device_id_type=MESH)
    for k in range(1, n_gy):
        pl.semaphore_signal(barrier, inc=1, device_id={"gy": lax.rem(gy + k, n_gy)}, device_id_type=MESH)
    expected = jnp.int32(n_gx - 1 + n_gy - 1)
    for d in diag:
        cond = exists(*d)

        @pl.when(cond)
        def _():
            pl.semaphore_signal(barrier, inc=1, device_id=target(*d), device_id_type=MESH)

        expected = expected + cond.astype(jnp.int32)

    lane = lax.broadcasted_iota(jnp.int32, (ROWS, LANES), 1)
    sub = lax.broadcasted_iota(jnp.int32, (ROWS, LANES), 0)

    def tile(ref, q, z):
        return ref[q, z]

    def strided(ref, q, zt, y):
        return ref[q, pl.ds(zt * ROWS, ROWS), y]

    for c in loads:
        c.wait()

    packed_sum = jnp.zeros((ROWS, LANES), jnp.float32)
    for zt in range(tiles):
        total = A[3, zt * ROWS:(zt + 1) * ROWS, 0]
        for y in range(1, ROWS):
            total = total + A[3, zt * ROWS:(zt + 1) * ROWS, y]
        packed_sum = jnp.where(lane == zt, jnp.sum(total, axis=1, keepdims=True), packed_sum)
    T0[...] = packed_sum

    group = lane // 4
    spot = lane % 4
    for q in range(5):
        def pack(z, carry):
            left, right = carry
            t = tile(A, q, z)
            here = jnp.logical_and(group == z, spot < 3)
            left = jnp.where(here, pltpu.roll(t, 4 * z, 1), left)
            right = jnp.where(here, pltpu.roll(t, lax.rem(4 * z + 3, LANES), 1), right)
            return left, right
        zero = jnp.zeros((ROWS, LANES), jnp.float32)
        left, right = lax.fori_loop(0, depth, pack, (zero, zero), unroll=8)
        SX[0, q] = left
        SX[1, q] = right

    pl.semaphore_wait(barrier, expected)

    moves = []

    def message(dx, dy, src, dst, ssem, rsem):
        c = pltpu.make_async_remote_copy(src_ref=src, dst_ref=dst, send_sem=ssem, recv_sem=rsem,
                                         device_id=target(dx, dy), device_id_type=MESH)
        send_if, recv_if = exists(dx, dy), exists(-dx, -dy)

        @pl.when(send_if)
        def _():
            c.start()

        moves.append((send_if, c))

        def arrive():
            @pl.when(recv_if)
            def _():
                c.wait_recv()

            @pl.when(jnp.logical_not(recv_if))
            def _():
                dst[...] = jnp.zeros(dst.shape, jnp.float32)

        return arrive

    y_arrive, x_arrive, d_arrive = [], [], []
    for side, dx in ((0, 1), (1, -1)):
        for j in range(3):
            row = ROWS - 3 + j if dx == 1 else j
            near = j == 2 if dx == 1 else j == 0
            count = 5 if near else 4
            y_arrive.append(message(dx, 0, fields.at[pl.ds(0, count), :, row], YH.at[side, j, pl.ds(0, count)],
                                    y_send.at[side, j], y_recv.at[side, j]))
    for side, dy in ((0, 1), (1, -1)):
        x_arrive.append(message(0, dy, SX.at[1 - side], RX.at[side], x_send.at[side], x_recv.at[side]))
    for i, (dx, dy) in enumerate(diag):
        a, b = (0 if dx == 1 else 1), (0 if dy == 1 else 1)
        row = ROWS - 1 if dx == 1 else 0
        d_arrive.append(message(dx, dy, fields.at[pl.ds(0, 2), :, row], DR.at[a, b], d_send.at[0, i], d_recv.at[0, i]))
        d_arrive.append(message(dx, dy, SX.at[1 - b, pl.ds(0, 2)], DP.at[a, b], d_send.at[1, i], d_recv.at[1, i]))
    stage1 = []
    for k in range(1, n_gx):
        c = pltpu.make_async_remote_copy(src_ref=T0, dst_ref=R1.at[k - 1], send_sem=t_send.at[k - 1],
                                         recv_sem=t_recv.at[k - 1],
                                         device_id={"gx": lax.rem(gx + k, n_gx)}, device_id_type=MESH)
        c.start()
        stage1.append(c)

    turning = jnp.zeros((ROWS, LANES), jnp.float32)
    for y in range(ROWS):
        turning = jnp.where(sub == y, coriolis[y], turning)
    turning = SECTION_DT * turning
    east_dt = HALF_DT * east[...]
    north_dt = HALF_DT * north[...]

    def vertical(z, lower):
        at = [jnp.clip(z + o, 0, depth - 1) for o in (-2, -1, 0, 1, 2, 3)]
        speed = HALF_DT * (tile(A, 2, z) + tile(A, 2, at[3]))
        speed = speed * (z < depth - 1).astype(jnp.float32)
        positive = speed > 0.0
        weight = jnp.abs(speed) * (1.0 / 6.0)
        pz = tile(A, 4, at[3]) - tile(A, 4, at[1])
        factor = 1.0 - (z.astype(jnp.float32) + 0.5) / depth
        u, v = tile(A, 0, z), tile(A, 1, z)
        scaled = pz * factor
        force = (scaled * east_dt + turning * v, scaled * north_dt - turning * u, -HALF_DT * pz, None)
        uppers = []
        for q in range(4):
            cells = [tile(A, q, a) for a in at]
            upper = weno_flux(cells, positive, speed, weight)
            value = cells[2] - (upper - lower[q])
            if force[q] is not None:
                value = value + force[q]
            acc[q, z] = value
            uppers.append(upper)
        return tuple(uppers)

    zero = jnp.zeros((ROWS, LANES), jnp.float32)
    lax.fori_loop(0, depth, vertical, (zero,) * 4)

    for c in stage1:
        c.wait_recv()
    summed = T0[...]
    for k in range(n_gx - 1):
        summed = summed + R1[k]
    T1[...] = summed
    stage2 = []
    for k in range(1, n_gy):
        c = pltpu.make_async_remote_copy(src_ref=T1, dst_ref=R2.at[k - 1], send_sem=s_send.at[k - 1],
                                         recv_sem=s_recv.at[k - 1],
                                         device_id={"gy": lax.rem(gy + k, n_gy)}, device_id_type=MESH)
        c.start()
        stage2.append(c)

    for arrive in x_arrive:
        arrive()

    def shift(x, j, axis=1):
        n = x.shape[axis]
        return pltpu.roll(x, (-j) % n, axis)

    extra = []
    u_last = shift(SX[1, 0], 2)
    speed_e = HALF_DT * (u_last + RX[1, 0])
    positive_e = speed_e > 0.0
    weight_e = jnp.abs(speed_e) * (1.0 / 6.0)
    for q in range(4):
        own, far = SX[1, q], RX[1, q]
        cells = [own, shift(own, 1), shift(own, 2), far, shift(far, 1), shift(far, 2)]
        extra.append(weno_flux(cells, positive_e, speed_e, weight_e))

    def horizontal(z, carry):
        to_low = lax.rem(2 * LANES - 4 * z - 3, LANES)
        to_high = lax.rem(LANES - 4 * z, LANES)

        def moved(q, t, low, high):
            rl = pltpu.roll(RX[0, q], to_low, 1)
            rr = pltpu.roll(RX[1, q], to_high, 1)
            down = [pltpu.roll(jnp.where(lane >= LANES - j, rl, t), j, 1) for j in range(low, 0, -1)]
            up = [pltpu.roll(jnp.where(lane < j, rr, t), LANES - j, 1) for j in range(1, high + 1)]
            return down + [t] + up

        speed = positive = weight = None
        for q in range(4):
            cells = moved(q, tile(A, q, z), 3, 2)
            if q == 0:
                speed = HALF_DT * (cells[2] + cells[3])
                positive = speed > 0.0
                weight = jnp.abs(speed) * (1.0 / 6.0)
                dux[z] = cells[4] - cells[2]
            if q == 1:
                dvx[z] = cells[4] - cells[2]
            flux = weno_flux(cells, positive, speed, weight)
            past = jnp.where(lane == 0, pltpu.roll(extra[q], to_high, 1), flux)
            change = pltpu.roll(past, LANES - 1, 1) - flux
            if q == 0:
                pcells = moved(4, tile(A, 4, z), 1, 1)
                change = change + HALF_DT * (pcells[2] - pcells[0])
            acc[q, z] = acc[q, z] - change
            dm[q, z] = cells[3] - cells[2]
            dp[q, z] = cells[4] - cells[3]
        return carry

    lax.fori_loop(0, depth, horizontal, 0)

    for arrive in y_arrive + d_arrive:
        arrive()
    for c in stage2:
        c.wait_recv()
    mean = T1[...]
    for k in range(n_gy - 1):
        mean = mean + R2[k]
    mean = mean * (1.0 / (ROWS * LANES * n_gx * n_gy))

    scale = HALF_DT * SMAG_COEF

    def mixing_coefficient(ux, vy, uy, vx):
        cross = uy + vx
        return scale * jnp.sqrt(0.5 * (ux * ux + vy * vy) + (0.25 * (cross * cross) + BACKGROUND))

    def along_y(zt, carry):
        levels = pl.ds(pl.multiple_of(zt * ROWS, ROWS), ROWS)

        def row(q, y):
            if y < 0:
                return YH[0, y + 3, q, levels]
            if y >= ROWS:
                return YH[1, y - ROWS, q, levels]
            return A[q, levels, y]

        us = {y: row(0, y) for y in range(-2, ROWS + 2)}
        vs = {y: row(1, y) for y in range(-2, ROWS + 2)}
        eddy = []
        for y in range(-1, ROWS + 1):
            if 0 <= y < ROWS:
                ux, vx = dux[levels, y], dvx[levels, y]
            else:
                a = 0 if y < 0 else 1
                both = []
                for q, base in ((0, us[y]), (1, vs[y])):
                    right = pltpu.roll(jnp.where(lane == 0, DR[a, 1, q, levels], base), LANES - 1, 1)
                    left = pltpu.roll(jnp.where(lane == LANES - 1, DR[a, 0, q, levels], base), 1, 1)
                    both.append(right - left)
                ux, vx = both
            e = mixing_coefficient(ux, vs[y + 1] - vs[y - 1], us[y + 1] - us[y - 1], vx)
            eddy.append(e)
            if 0 <= y < ROWS:
                EA[levels, y] = e
        speeds, signs, weights, spread = [], [], [], []
        for f in range(ROWS + 1):
            s = HALF_DT * (vs[f - 1] + vs[f])
            speeds.append(s)
            signs.append(s > 0.0)
            weights.append(jnp.abs(s) * (1.0 / 6.0))
            spread.append(eddy[f] + eddy[f + 1])
        level_mean = jnp.sum(jnp.where(lane == zt, mean, 0.0), axis=1, keepdims=True)
        for q in range(4):
            cells = [row(q, y) for y in range(-3, ROWS + 3)]
            lower = None
            for f in range(ROWS + 1):
                six = cells[f:f + 6]
                flux = weno_flux(six, signs[f], speeds[f], weights[f]) - spread[f] * (six[3] - six[2])
                if f:
                    y = f - 1
                    value = acc[q, levels, y] - (flux - lower)
                    if q == 1:
                        value = value - HALF_DT * (row(4, y + 1) - row(4, y - 1))
                    if q == 2:
                        value = value + (SECTION_DT * BUOYANCY) * (row(3, y) - level_mean)
                    acc[q, levels, y] = value
                lower = flux
        return carry

    lax.fori_loop(0, tiles, along_y, 0)

    def outside(side):
        parts = []
        for q in range(2):
            far, own = RX[side, q], SX[side, q]
            if side == 0:
                plus, base, minus = own, shift(far, 2), shift(far, 1)
                above, below = shift(DP[1, 0, q], 2), shift(DP[0, 0, q], 2)
            else:
                plus, base, minus = shift(far, 1), far, shift(own, 2)
                above, below = DP[1, 1, q], DP[0, 1, q]
            nxt = pltpu.roll(jnp.where(sub == 0, above, base), ROWS - 1, 0)
            prv = pltpu.roll(jnp.where(sub == ROWS - 1, below, base), 1, 0)
            parts.append((plus - minus, nxt - prv))
        (ux, uy), (vx, vy) = parts
        return mixing_coefficient(ux, vy, uy, vx)

    e_low, e_high = outside(0), outside(1)

    def final(z, carry):
        e = EA[z]
        low = pltpu.roll(e_low, lax.rem(2 * LANES - 4 * z - 1, LANES), 1)
        high = pltpu.roll(e_high, lax.rem(LANES - 4 * z, LANES), 1)
        before = e + pltpu.roll(jnp.where(lane == LANES - 1, low, e), 1, 1)
        after = e + pltpu.roll(jnp.where(lane == 0, high, e), LANES - 1, 1)
        for q in range(4):
            out[q, z] = acc[q, z] + (after * dp[q, z] - before * dm[q, z])
        return carry

    lax.fori_loop(0, depth, final, 0, unroll=4)

    for cond, c in moves:
        @pl.when(cond)
        def _():
            c.wait_send()
    for c in stage1 + stage2:
        c.wait_send()


def body(n_gx, n_gy, fields, coriolis, slope_east, slope_north):
    depth = fields.shape[1]
    f32 = jnp.float32
    block = (depth, ROWS, LANES)
    dma = pltpu.SemaphoreType.DMA
    vmem = pl.BlockSpec(memory_space=pltpu.VMEM)
    return pl.pallas_call(
        functools.partial(kernel, n_gx, n_gy, depth),
        out_shape=jax.ShapeDtypeStruct((4,) + block, f32),
        in_specs=[pl.BlockSpec(memory_space=pl.ANY), pl.BlockSpec(memory_space=pltpu.SMEM), vmem, vmem],
        out_specs=vmem,
        scratch_shapes=[
            pltpu.VMEM((5,) + block, f32),
            pltpu.VMEM((4,) + block, f32),
            pltpu.VMEM((4,) + block, f32),
            pltpu.VMEM((4,) + block, f32),
            pltpu.VMEM(block, f32),
            pltpu.VMEM(block, f32),
            pltpu.VMEM(block, f32),
            pltpu.VMEM((2, 5, ROWS, LANES), f32),
            pltpu.VMEM((2, 5, ROWS, LANES), f32),
            pltpu.VMEM((2, 3, 5, depth, LANES), f32),
            pltpu.VMEM((2, 2, 2, depth, LANES), f32),
            pltpu.VMEM((2, 2, 2, ROWS, LANES), f32),
            pltpu.VMEM((ROWS, LANES), f32),
            pltpu.VMEM((ROWS, LANES), f32),
            pltpu.VMEM((n_gx - 1, ROWS, LANES), f32),
            pltpu.VMEM((n_gy - 1, ROWS, LANES), f32),
            dma((5,)),
            dma((2, 3)), dma((2, 3)),
            dma((2,)), dma((2,)),
            dma((2, 4)), dma((2, 4)),
            dma((n_gx - 1,)), dma((n_gx - 1,)),
            dma((n_gy - 1,)), dma((n_gy - 1,)),
        ],
        compiler_params=pltpu.CompilerParams(collective_id=0, has_side_effects=True),
        name="section",
    )(fields, coriolis, slope_east, slope_north)


def solution(mesh):
    return jax.shard_map(
        functools.partial(body, mesh.shape["gx"], mesh.shape["gy"]),
        mesh=mesh,
        in_specs=(P(None, None, "gx", "gy"), P("gx"), P("gx", "gy"), P("gx", "gy")),
        out_specs=P(None, None, "gx", "gy"),
        check_vma=False,
    )
```

```python
import functools

import jax
import jax.numpy as jnp
from jax import lax
from jax.experimental import pallas as pl
from jax.experimental.pallas import tpu as pltpu
from jax.sharding import PartitionSpec as P

WENO_EPS = 1e-06
SECTION_DT = 0.3
SMAG_COEF = 0.06
BACKGROUND = 0.05
BUOYANCY = 0.5
MESH = pl.DeviceIdType.MESH
HALF_DT = 0.5 * SECTION_DT
LANES = 128
ROWS = 8


def weno_flux(cells, positive, speed, weight):
    q0, q1, q2, q3, q4, q5 = cells
    d0, d1, d2, d3, d4 = q1 - q0, q2 - q1, q3 - q2, q4 - q3, q5 - q4
    e1 = jnp.where(positive, d0, d4)
    e2 = jnp.where(positive, d1, d3)
    e3 = d2
    e4 = jnp.where(positive, d3, d1)
    centre = jnp.where(positive, q2, q3)
    sa, sb, sc = e2 - e1, e3 - e2, e4 - e3
    eps = 4.0 * WENO_EPS
    k = 13.0 / 3.0
    x0 = 3.0 * e2 - e1
    x1 = e2 + e3
    x2 = 3.0 * e3 - e4
    y0 = (k * sa) * sa + (x0 * x0 + eps)
    y1 = (k * sb) * sb + (x1 * x1 + eps)
    y2 = (k * sc) * sc + (x2 * x2 + eps)
    m0, m1, m2 = y1 * y2, y0 * y2, y0 * y1
    w0 = m0 * m0
    w1 = 6.0 * (m1 * m1)
    w2 = 3.0 * (m2 * m2)
    bottom = w0 + w1 + w2
    first = w0 * (sb - sa)
    top = first + first + w2 * (sc - sb)
    return speed * centre + weight * ((x1 + e3) - top / bottom)


def kernel(n_gx, n_gy, depth, fields, coriolis, east, north, out,
           A, acc, dm, dp, dux, dvx, EA, SX, RX, YS, YH, DS, DR, MB, T0, T1, R1, R2,
           in_sem, y_send, y_recv, x_send, x_recv, d_send, d_recv, t_send, t_recv, s_send, s_recv):
    gx = lax.axis_index("gx")
    gy = lax.axis_index("gy")
    tiles = depth // ROWS
    diag = [(1, 1), (1, -1), (-1, 1), (-1, -1)]

    def exists(dx, dy):
        cond = None
        for pos, d, n in ((gx, dx, n_gx), (gy, dy, n_gy)):
            if d == 0:
                continue
            c = (pos + d < n) if d > 0 else (pos + d >= 0)
            cond = c if cond is None else jnp.logical_and(cond, c)
        return cond

    def target(dx, dy):
        return {"gx": gx + dx, "gy": gy + dy}

    loads = []
    for q in (3, 0, 1, 2, 4):
        c = pltpu.make_async_copy(fields.at[q], A.at[q], in_sem.at[q])
        c.start()
        loads.append(c)

    barrier = pltpu.get_barrier_semaphore()
    for k in range(1, n_gx):
        pl.semaphore_signal(barrier, inc=1, device_id={"gx": lax.rem(gx + k, n_gx)}, device_id_type=MESH)
    for k in range(1, n_gy):
        pl.semaphore_signal(barrier, inc=1, device_id={"gy": lax.rem(gy + k, n_gy)}, device_id_type=MESH)
    expected = jnp.int32(n_gx - 1 + n_gy - 1)
    for d in diag:
        cond = exists(*d)

        @pl.when(cond)
        def _():
            pl.semaphore_signal(barrier, inc=1, device_id=target(*d), device_id_type=MESH)

        expected = expected + cond.astype(jnp.int32)

    lane = lax.broadcasted_iota(jnp.int32, (ROWS, LANES), 1)
    sub = lax.broadcasted_iota(jnp.int32, (ROWS, LANES), 0)

    def tile(ref, q, z):
        return ref[q, z]

    flat4 = lambda ref: ref.reshape(ref.shape[0], depth * ROWS, LANES)
    flat3 = lambda ref: ref.reshape(depth * ROWS, LANES)
    Af, accf, duxf, dvxf, EAf = flat4(A), flat4(acc), flat3(dux), flat3(dvx), flat3(EA)

    def every(zt, y):
        return pl.ds(zt * ROWS * ROWS + y, ROWS, stride=ROWS)

    for c in loads:
        c.wait()

    packed_sum = jnp.zeros((ROWS, LANES), jnp.float32)
    for zt in range(tiles):
        total = Af[3, every(zt, 0)]
        for y in range(1, ROWS):
            total = total + Af[3, every(zt, y)]
        packed_sum = jnp.where(lane == zt, jnp.sum(total, axis=1, keepdims=True), packed_sum)
    T0[...] = packed_sum

    group = lane // 4
    spot = lane % 4
    for q in range(5):
        def pack(z, carry):
            left, right = carry
            t = tile(A, q, z)
            here = jnp.logical_and(group == z, spot < 3)
            left = jnp.where(here, pltpu.roll(t, 4 * z, 1), left)
            right = jnp.where(here, pltpu.roll(t, lax.rem(4 * z + 3, LANES), 1), right)
            return left, right
        zero = jnp.zeros((ROWS, LANES), jnp.float32)
        left, right = lax.fori_loop(0, depth, pack, (zero, zero), unroll=8)
        SX[0, q] = left
        SX[1, q] = right

    def slot(j, q):
        return 4 * j + q if q < 4 else 12

    for side in range(2):
        near = 0 if side == 0 else ROWS - 1
        for q in range(5):
            for j in (range(3) if q < 4 else (0,)):
                row = near + j if side == 0 else near - j
                for zt in range(tiles):
                    YS[side, slot(j, q), zt * ROWS:(zt + 1) * ROWS] = Af[q, every(zt, row)]

    for a in range(2):
        row = ROWS - 1 if a == 0 else 0
        for b in range(2):
            column = LANES - 1 if b == 0 else 0
            packed = jnp.zeros((ROWS, LANES), jnp.float32)
            for zt in range(tiles):
                for q in range(2):
                    t = Af[q, every(zt, row)]
                    goal = 2 * zt + q
                    packed = jnp.where(lane == goal, pltpu.roll(t, (goal - column) % LANES, 1), packed)
            DS[a, b, 0] = packed
            DS[a, b, 1] = SX[1 - b, 0]
            DS[a, b, 2] = SX[1 - b, 1]

    pl.semaphore_wait(barrier, expected)

    moves = []

    def message(dx, dy, src, dst, ssem, rsem):
        c = pltpu.make_async_remote_copy(src_ref=src, dst_ref=dst, send_sem=ssem, recv_sem=rsem,
                                         device_id=target(dx, dy), device_id_type=MESH)
        send_if, recv_if = exists(dx, dy), exists(-dx, -dy)

        @pl.when(send_if)
        def _():
            c.start()

        moves.append((send_if, c))

        def arrive():
            @pl.when(recv_if)
            def _():
                c.wait_recv()

            @pl.when(jnp.logical_not(recv_if))
            def _():
                dst[...] = jnp.zeros(dst.shape, jnp.float32)

        return arrive

    y_arrive, x_arrive, d_arrive = [], [], []
    for side, dx in ((0, 1), (1, -1)):
        y_arrive.append(message(dx, 0, YS.at[1 - side], YH.at[side], y_send.at[side], y_recv.at[side]))
    for side, dy in ((0, 1), (1, -1)):
        x_arrive.append(message(0, dy, SX.at[1 - side], RX.at[side], x_send.at[side], x_recv.at[side]))
    for i, (dx, dy) in enumerate(diag):
        a, b = (0 if dx == 1 else 1), (0 if dy == 1 else 1)
        d_arrive.append(message(dx, dy, DS.at[a, b], DR.at[a, b], d_send.at[i], d_recv.at[i]))
    stage1 = []
    for k in range(1, n_gx):
        c = pltpu.make_async_remote_copy(src_ref=T0, dst_ref=R1.at[k - 1], send_sem=t_send.at[k - 1],
                                         recv_sem=t_recv.at[k - 1],
                                         device_id={"gx": lax.rem(gx + k, n_gx)}, device_id_type=MESH)
        c.start()
        stage1.append(c)

    turning = jnp.zeros((ROWS, LANES), jnp.float32)
    for y in range(ROWS):
        turning = jnp.where(sub == y, coriolis[y], turning)
    turning = SECTION_DT * turning
    east_dt = HALF_DT * east[...]
    north_dt = HALF_DT * north[...]

    def vertical(z, lower):
        at = [jnp.clip(z + o, 0, depth - 1) for o in (-2, -1, 0, 1, 2, 3)]
        speed = HALF_DT * (tile(A, 2, z) + tile(A, 2, at[3]))
        speed = speed * (z < depth - 1).astype(jnp.float32)
        positive = speed > 0.0
        weight = jnp.abs(speed) * (1.0 / 6.0)
        pz = tile(A, 4, at[3]) - tile(A, 4, at[1])
        factor = 1.0 - (z.astype(jnp.float32) + 0.5) / depth
        u, v = tile(A, 0, z), tile(A, 1, z)
        scaled = pz * factor
        force = (scaled * east_dt + turning * v, scaled * north_dt - turning * u, -HALF_DT * pz, None)
        uppers = []
        for q in range(4):
            cells = [tile(A, q, a) for a in at]
            upper = weno_flux(cells, positive, speed, weight)
            value = cells[2] - (upper - lower[q])
            if force[q] is not None:
                value = value + force[q]
            acc[q, z] = value
            uppers.append(upper)
        return tuple(uppers)

    zero = jnp.zeros((ROWS, LANES), jnp.float32)
    lax.fori_loop(0, depth, vertical, (zero,) * 4)

    for c in stage1:
        c.wait_recv()
    summed = T0[...]
    for k in range(n_gx - 1):
        summed = summed + R1[k]
    T1[...] = summed
    stage2 = []
    for k in range(1, n_gy):
        c = pltpu.make_async_remote_copy(src_ref=T1, dst_ref=R2.at[k - 1], send_sem=s_send.at[k - 1],
                                         recv_sem=s_recv.at[k - 1],
                                         device_id={"gy": lax.rem(gy + k, n_gy)}, device_id_type=MESH)
        c.start()
        stage2.append(c)

    for arrive in x_arrive:
        arrive()

    def shift(x, j, axis=1):
        n = x.shape[axis]
        return pltpu.roll(x, (-j) % n, axis)

    extra = []
    u_last = shift(SX[1, 0], 2)
    speed_e = HALF_DT * (u_last + RX[1, 0])
    positive_e = speed_e > 0.0
    weight_e = jnp.abs(speed_e) * (1.0 / 6.0)
    for q in range(4):
        own, far = SX[1, q], RX[1, q]
        cells = [own, shift(own, 1), shift(own, 2), far, shift(far, 1), shift(far, 2)]
        extra.append(weno_flux(cells, positive_e, speed_e, weight_e))

    def horizontal(z, carry):
        to_low = lax.rem(2 * LANES - 4 * z - 3, LANES)
        to_high = lax.rem(LANES - 4 * z, LANES)

        def moved(q, t, low, high):
            rl = pltpu.roll(RX[0, q], to_low, 1)
            rr = pltpu.roll(RX[1, q], to_high, 1)
            down = [pltpu.roll(jnp.where(lane >= LANES - j, rl, t), j, 1) for j in range(low, 0, -1)]
            up = [pltpu.roll(jnp.where(lane < j, rr, t), LANES - j, 1) for j in range(1, high + 1)]
            return down + [t] + up

        speed = positive = weight = None
        for q in range(4):
            cells = moved(q, tile(A, q, z), 3, 2)
            if q == 0:
                speed = HALF_DT * (cells[2] + cells[3])
                positive = speed > 0.0
                weight = jnp.abs(speed) * (1.0 / 6.0)
                dux[z] = cells[4] - cells[2]
            if q == 1:
                dvx[z] = cells[4] - cells[2]
            flux = weno_flux(cells, positive, speed, weight)
            past = jnp.where(lane == 0, pltpu.roll(extra[q], to_high, 1), flux)
            change = pltpu.roll(past, LANES - 1, 1) - flux
            if q == 0:
                pcells = moved(4, tile(A, 4, z), 1, 1)
                change = change + HALF_DT * (pcells[2] - pcells[0])
            acc[q, z] = acc[q, z] - change
            dm[q, z] = cells[3] - cells[2]
            dp[q, z] = cells[4] - cells[3]
        return carry

    lax.fori_loop(0, depth, horizontal, 0)

    for arrive in y_arrive + d_arrive:
        arrive()
    scale = HALF_DT * SMAG_COEF

    def mixing_coefficient(ux, vy, uy, vx):
        cross = uy + vx
        return scale * jnp.sqrt(0.5 * (ux * ux + vy * vy) + (0.25 * (cross * cross) + BACKGROUND))

    def along_y(zt, carry):
        levels = pl.ds(pl.multiple_of(zt * ROWS, ROWS), ROWS)

        def row(q, y):
            if y < 0:
                return YH[0, slot(-1 - y, q), levels]
            if y >= ROWS:
                return YH[1, slot(y - ROWS, q), levels]
            return Af[q, every(zt, y)]

        us = {y: row(0, y) for y in range(-2, ROWS + 2)}
        vs = {y: row(1, y) for y in range(-2, ROWS + 2)}
        eddy = []
        for y in range(-1, ROWS + 1):
            if 0 <= y < ROWS:
                ux, vx = duxf[every(zt, y)], dvxf[every(zt, y)]
            else:
                a = 0 if y < 0 else 1
                both = []
                for q, base in ((0, us[y]), (1, vs[y])):
                    right = pltpu.roll(jnp.where(lane == 0, pltpu.roll(DR[a, 1, 0], lax.rem(LANES - 2 * zt - q, LANES), 1), base), LANES - 1, 1)
                    left = pltpu.roll(jnp.where(lane == LANES - 1, pltpu.roll(DR[a, 0, 0], LANES - 1 - 2 * zt - q, 1), base), 1, 1)
                    both.append(right - left)
                ux, vx = both
            e = mixing_coefficient(ux, vs[y + 1] - vs[y - 1], us[y + 1] - us[y - 1], vx)
            eddy.append(e)
            if 0 <= y < ROWS:
                EAf[every(zt, y)] = e
        speeds, signs, weights, spread = [], [], [], []
        for f in range(ROWS + 1):
            s = HALF_DT * (vs[f - 1] + vs[f])
            speeds.append(s)
            signs.append(s > 0.0)
            weights.append(jnp.abs(s) * (1.0 / 6.0))
            spread.append(eddy[f] + eddy[f + 1])
        for q in range(4):
            cells = [row(q, y) for y in range(-3, ROWS + 3)]
            lower = None
            for f in range(ROWS + 1):
                six = cells[f:f + 6]
                flux = weno_flux(six, signs[f], speeds[f], weights[f]) - spread[f] * (six[3] - six[2])
                if f:
                    y = f - 1
                    value = accf[q, every(zt, y)] - (flux - lower)
                    if q == 1:
                        value = value - HALF_DT * (row(4, y + 1) - row(4, y - 1))
                    if q == 2:
                        value = value + (SECTION_DT * BUOYANCY) * row(3, y)
                    accf[q, every(zt, y)] = value
                lower = flux
        return carry

    lax.fori_loop(0, tiles, along_y, 0)

    def outside(side):
        parts = []
        for q in range(2):
            far, own = RX[side, q], SX[side, q]
            if side == 0:
                plus, base, minus = own, shift(far, 2), shift(far, 1)
                above, below = shift(DR[1, 0, q + 1], 2), shift(DR[0, 0, q + 1], 2)
            else:
                plus, base, minus = shift(far, 1), far, shift(own, 2)
                above, below = DR[1, 1, q + 1], DR[0, 1, q + 1]
            nxt = pltpu.roll(jnp.where(sub == 0, above, base), ROWS - 1, 0)
            prv = pltpu.roll(jnp.where(sub == ROWS - 1, below, base), 1, 0)
            parts.append((plus - minus, nxt - prv))
        (ux, uy), (vx, vy) = parts
        return mixing_coefficient(ux, vy, uy, vx)

    e_low, e_high = outside(0), outside(1)

    for c in stage2:
        c.wait_recv()
    mean = T1[...]
    for k in range(n_gy - 1):
        mean = mean + R2[k]
    mean = mean * (1.0 / (ROWS * LANES * n_gx * n_gy))
    mean = (SECTION_DT * BUOYANCY) * mean
    for zt in range(tiles):
        level = jnp.sum(jnp.where(lane == zt, mean, 0.0), axis=1, keepdims=True)
        MB[zt * ROWS:(zt + 1) * ROWS] = jnp.broadcast_to(level, (ROWS, LANES))

    def final(z, carry):
        e = EA[z]
        low = pltpu.roll(e_low, lax.rem(2 * LANES - 4 * z - 1, LANES), 1)
        high = pltpu.roll(e_high, lax.rem(LANES - 4 * z, LANES), 1)
        before = e + pltpu.roll(jnp.where(lane == LANES - 1, low, e), 1, 1)
        after = e + pltpu.roll(jnp.where(lane == 0, high, e), LANES - 1, 1)
        for q in range(4):
            value = acc[q, z] + (after * dp[q, z] - before * dm[q, z])
            if q == 2:
                value = value - MB[pl.ds(z, 1)]
            out[q, z] = value
        return carry

    lax.fori_loop(0, depth, final, 0, unroll=4)

    for cond, c in moves:
        @pl.when(cond)
        def _():
            c.wait_send()
    for c in stage1 + stage2:
        c.wait_send()


def body(n_gx, n_gy, fields, coriolis, slope_east, slope_north):
    depth = fields.shape[1]
    f32 = jnp.float32
    block = (depth, ROWS, LANES)
    dma = pltpu.SemaphoreType.DMA
    vmem = pl.BlockSpec(memory_space=pltpu.VMEM)
    return pl.pallas_call(
        functools.partial(kernel, n_gx, n_gy, depth),
        out_shape=jax.ShapeDtypeStruct((4,) + block, f32),
        in_specs=[pl.BlockSpec(memory_space=pl.ANY), pl.BlockSpec(memory_space=pltpu.SMEM), vmem, vmem],
        out_specs=vmem,
        scratch_shapes=[
            pltpu.VMEM((5,) + block, f32),
            pltpu.VMEM((4,) + block, f32),
            pltpu.VMEM((4,) + block, f32),
            pltpu.VMEM((4,) + block, f32),
            pltpu.VMEM(block, f32),
            pltpu.VMEM(block, f32),
            pltpu.VMEM(block, f32),
            pltpu.VMEM((2, 5, ROWS, LANES), f32),
            pltpu.VMEM((2, 5, ROWS, LANES), f32),
            pltpu.VMEM((2, 13, depth, LANES), f32),
            pltpu.VMEM((2, 13, depth, LANES), f32),
            pltpu.VMEM((2, 2, 3, ROWS, LANES), f32),
            pltpu.VMEM((2, 2, 3, ROWS, LANES), f32),
            pltpu.VMEM((depth, LANES), f32),
            pltpu.VMEM((ROWS, LANES), f32),
            pltpu.VMEM((ROWS, LANES), f32),
            pltpu.VMEM((n_gx - 1, ROWS, LANES), f32),
            pltpu.VMEM((n_gy - 1, ROWS, LANES), f32),
            dma((5,)),
            dma((2,)), dma((2,)),
            dma((2,)), dma((2,)),
            dma((4,)), dma((4,)),
            dma((n_gx - 1,)), dma((n_gx - 1,)),
            dma((n_gy - 1,)), dma((n_gy - 1,)),
        ],
        compiler_params=pltpu.CompilerParams(collective_id=0, has_side_effects=True),
        name="section",
    )(fields, coriolis, slope_east, slope_north)


def solution(mesh):
    return jax.shard_map(
        functools.partial(body, mesh.shape["gx"], mesh.shape["gy"]),
        mesh=mesh,
        in_specs=(P(None, None, "gx", "gy"), P("gx"), P("gx", "gy"), P("gx", "gy")),
        out_specs=P(None, None, "gx", "gy"),
        check_vma=False,
    )
```

```python
import functools

import jax
import jax.numpy as jnp
from jax import lax
from jax.experimental import pallas as pl
from jax.experimental.pallas import tpu as pltpu
from jax.sharding import PartitionSpec as P

WENO_EPS = 1e-06
SECTION_DT = 0.3
SMAG_COEF = 0.06
BACKGROUND = 0.05
BUOYANCY = 0.5
MESH = pl.DeviceIdType.MESH
HALF_DT = 0.5 * SECTION_DT
LANES = 128
ROWS = 8


def weno_flux(cells, positive, speed, weight):
    q0, q1, q2, q3, q4, q5 = cells
    d0, d1, d2, d3, d4 = q1 - q0, q2 - q1, q3 - q2, q4 - q3, q5 - q4
    e1 = jnp.where(positive, d0, d4)
    e2 = jnp.where(positive, d1, d3)
    e3 = d2
    e4 = jnp.where(positive, d3, d1)
    centre = jnp.where(positive, q2, q3)
    sa, sb, sc = e2 - e1, e3 - e2, e4 - e3
    eps = 4.0 * WENO_EPS
    k = 13.0 / 3.0
    x0 = 3.0 * e2 - e1
    x1 = e2 + e3
    x2 = 3.0 * e3 - e4
    y0 = (k * sa) * sa + (x0 * x0 + eps)
    y1 = (k * sb) * sb + (x1 * x1 + eps)
    y2 = (k * sc) * sc + (x2 * x2 + eps)
    m0, m1, m2 = y1 * y2, y0 * y2, y0 * y1
    w0 = m0 * m0
    w1 = 6.0 * (m1 * m1)
    w2 = 3.0 * (m2 * m2)
    bottom = w0 + w1 + w2
    first = w0 * (sb - sa)
    top = first + first + w2 * (sc - sb)
    return speed * centre + weight * ((x1 + e3) - top / bottom)


def kernel(n_gx, n_gy, depth, fields, coriolis, east, north, out,
           A, acc, dm, dp, dux, dvx, EA, SX, RX, YS, YH, DS, DR, MB, T0, T1, R1, R2,
           in_sem, y_send, y_recv, x_send, x_recv, d_send, d_recv, t_send, t_recv, s_send, s_recv):
    gx = lax.axis_index("gx")
    gy = lax.axis_index("gy")
    tiles = depth // ROWS
    diag = [(1, 1), (1, -1), (-1, 1), (-1, -1)]

    def exists(dx, dy):
        cond = None
        for pos, d, n in ((gx, dx, n_gx), (gy, dy, n_gy)):
            if d == 0:
                continue
            c = (pos + d < n) if d > 0 else (pos + d >= 0)
            cond = c if cond is None else jnp.logical_and(cond, c)
        return cond

    def target(dx, dy):
        return {"gx": gx + dx, "gy": gy + dy}

    loads = []
    for q in (3, 0, 1, 2, 4):
        c = pltpu.make_async_copy(fields.at[q], A.at[q], in_sem.at[q])
        c.start()
        loads.append(c)

    barrier = pltpu.get_barrier_semaphore()
    for k in range(1, n_gx):
        pl.semaphore_signal(barrier, inc=1, device_id={"gx": lax.rem(gx + k, n_gx)}, device_id_type=MESH)
    for k in range(1, n_gy):
        pl.semaphore_signal(barrier, inc=1, device_id={"gy": lax.rem(gy + k, n_gy)}, device_id_type=MESH)
    expected = jnp.int32(n_gx - 1 + n_gy - 1)
    for d in diag:
        cond = exists(*d)

        @pl.when(cond)
        def _():
            pl.semaphore_signal(barrier, inc=1, device_id=target(*d), device_id_type=MESH)

        expected = expected + cond.astype(jnp.int32)

    lane = lax.broadcasted_iota(jnp.int32, (ROWS, LANES), 1)
    sub = lax.broadcasted_iota(jnp.int32, (ROWS, LANES), 0)

    def tile(ref, q, z):
        return ref[q, z]

    flat4 = lambda ref: ref.reshape(ref.shape[0], depth * ROWS, LANES)
    flat3 = lambda ref: ref.reshape(depth * ROWS, LANES)
    Af, accf, duxf, dvxf, EAf = flat4(A), flat4(acc), flat3(dux), flat3(dvx), flat3(EA)

    def every(zt, y):
        return pl.ds(zt * ROWS * ROWS + y, ROWS, stride=ROWS)

    for c in loads:
        c.wait()

    packed_sum = jnp.zeros((ROWS, LANES), jnp.float32)
    for zt in range(tiles):
        total = Af[3, every(zt, 0)]
        for y in range(1, ROWS):
            total = total + Af[3, every(zt, y)]
        packed_sum = jnp.where(lane == zt, jnp.sum(total, axis=1, keepdims=True), packed_sum)
    T0[...] = packed_sum

    group = lane // 4
    spot = lane % 4
    for q in range(5):
        def pack(z, carry):
            left, right = carry
            t = tile(A, q, z)
            here = jnp.logical_and(group == z, spot < 3)
            left = jnp.where(here, pltpu.roll(t, 4 * z, 1), left)
            right = jnp.where(here, pltpu.roll(t, lax.rem(4 * z + 3, LANES), 1), right)
            return left, right
        zero = jnp.zeros((ROWS, LANES), jnp.float32)
        left, right = lax.fori_loop(0, depth, pack, (zero, zero), unroll=8)
        SX[0, q] = left
        SX[1, q] = right

    def slot(j, q):
        return 4 * j + q if q < 4 else 12

    for side in range(2):
        near = 0 if side == 0 else ROWS - 1
        for q in range(5):
            for j in (range(3) if q < 4 else (0,)):
                row = near + j if side == 0 else near - j
                for zt in range(tiles):
                    YS[side, slot(j, q), zt * ROWS:(zt + 1) * ROWS] = Af[q, every(zt, row)]

    for a in range(2):
        row = ROWS - 1 if a == 0 else 0
        for b in range(2):
            column = LANES - 1 if b == 0 else 0
            packed = jnp.zeros((ROWS, LANES), jnp.float32)
            for zt in range(tiles):
                for q in range(2):
                    t = Af[q, every(zt, row)]
                    goal = 2 * zt + q
                    packed = jnp.where(lane == goal, pltpu.roll(t, (goal - column) % LANES, 1), packed)
            DS[a, b, 0] = packed
            DS[a, b, 1] = SX[1 - b, 0]
            DS[a, b, 2] = SX[1 - b, 1]

    turning = jnp.zeros((ROWS, LANES), jnp.float32)
    for y in range(ROWS):
        turning = jnp.where(sub == y, coriolis[y], turning)
    turning = SECTION_DT * turning
    east_dt = HALF_DT * east[...]
    north_dt = HALF_DT * north[...]

    def vertical(z, lower):
        at = [jnp.clip(z + o, 0, depth - 1) for o in (-2, -1, 0, 1, 2, 3)]
        speed = HALF_DT * (tile(A, 2, z) + tile(A, 2, at[3]))
        speed = speed * (z < depth - 1).astype(jnp.float32)
        positive = speed > 0.0
        weight = jnp.abs(speed) * (1.0 / 6.0)
        pz = tile(A, 4, at[3]) - tile(A, 4, at[1])
        factor = 1.0 - (z.astype(jnp.float32) + 0.5) / depth
        u, v = tile(A, 0, z), tile(A, 1, z)
        scaled = pz * factor
        force = (scaled * east_dt + turning * v, scaled * north_dt - turning * u, -HALF_DT * pz, None)
        uppers = []
        for q in range(4):
            cells = [tile(A, q, a) for a in at]
            upper = weno_flux(cells, positive, speed, weight)
            value = cells[2] - (upper - lower[q])
            if force[q] is not None:
                value = value + force[q]
            acc[q, z] = value
            uppers.append(upper)
        return tuple(uppers)

    zero = jnp.zeros((ROWS, LANES), jnp.float32)
    lax.fori_loop(0, depth, vertical, (zero,) * 4)

    pl.semaphore_wait(barrier, expected)

    moves = []

    def message(dx, dy, src, dst, ssem, rsem):
        c = pltpu.make_async_remote_copy(src_ref=src, dst_ref=dst, send_sem=ssem, recv_sem=rsem,
                                         device_id=target(dx, dy), device_id_type=MESH)
        send_if, recv_if = exists(dx, dy), exists(-dx, -dy)

        @pl.when(send_if)
        def _():
            c.start()

        moves.append((send_if, c))

        def arrive():
            @pl.when(recv_if)
            def _():
                c.wait_recv()

            @pl.when(jnp.logical_not(recv_if))
            def _():
                dst[...] = jnp.zeros(dst.shape, jnp.float32)

        return arrive

    stage1 = []
    for k in range(1, n_gx):
        c = pltpu.make_async_remote_copy(src_ref=T0, dst_ref=R1.at[k - 1], send_sem=t_send.at[k - 1],
                                         recv_sem=t_recv.at[k - 1],
                                         device_id={"gx": lax.rem(gx + k, n_gx)}, device_id_type=MESH)
        c.start()
        stage1.append(c)

    y_arrive, x_arrive, d_arrive = [], [], []
    for side, dx in ((0, 1), (1, -1)):
        y_arrive.append(message(dx, 0, YS.at[1 - side], YH.at[side], y_send.at[side], y_recv.at[side]))
    for side, dy in ((0, 1), (1, -1)):
        x_arrive.append(message(0, dy, SX.at[1 - side], RX.at[side], x_send.at[side], x_recv.at[side]))
    for i, (dx, dy) in enumerate(diag):
        a, b = (0 if dx == 1 else 1), (0 if dy == 1 else 1)
        d_arrive.append(message(dx, dy, DS.at[a, b], DR.at[a, b], d_send.at[i], d_recv.at[i]))
    for c in stage1:
        c.wait_recv()
    summed = T0[...]
    for k in range(n_gx - 1):
        summed = summed + R1[k]
    T1[...] = summed
    stage2 = []
    for k in range(1, n_gy):
        c = pltpu.make_async_remote_copy(src_ref=T1, dst_ref=R2.at[k - 1], send_sem=s_send.at[k - 1],
                                         recv_sem=s_recv.at[k - 1],
                                         device_id={"gy": lax.rem(gy + k, n_gy)}, device_id_type=MESH)
        c.start()
        stage2.append(c)

    for arrive in x_arrive:
        arrive()

    def shift(x, j, axis=1):
        n = x.shape[axis]
        return pltpu.roll(x, (-j) % n, axis)

    extra = []
    u_last = shift(SX[1, 0], 2)
    speed_e = HALF_DT * (u_last + RX[1, 0])
    positive_e = speed_e > 0.0
    weight_e = jnp.abs(speed_e) * (1.0 / 6.0)
    for q in range(4):
        own, far = SX[1, q], RX[1, q]
        cells = [own, shift(own, 1), shift(own, 2), far, shift(far, 1), shift(far, 2)]
        extra.append(weno_flux(cells, positive_e, speed_e, weight_e))

    def horizontal(z, carry):
        to_low = lax.rem(2 * LANES - 4 * z - 3, LANES)
        to_high = lax.rem(LANES - 4 * z, LANES)

        def moved(q, t, low, high):
            rl = pltpu.roll(RX[0, q], to_low, 1)
            rr = pltpu.roll(RX[1, q], to_high, 1)
            down = [pltpu.roll(jnp.where(lane >= LANES - j, rl, t), j, 1) for j in range(low, 0, -1)]
            up = [pltpu.roll(jnp.where(lane < j, rr, t), LANES - j, 1) for j in range(1, high + 1)]
            return down + [t] + up

        speed = positive = weight = None
        for q in range(4):
            cells = moved(q, tile(A, q, z), 3, 2)
            if q == 0:
                speed = HALF_DT * (cells[2] + cells[3])
                positive = speed > 0.0
                weight = jnp.abs(speed) * (1.0 / 6.0)
                dux[z] = cells[4] - cells[2]
            if q == 1:
                dvx[z] = cells[4] - cells[2]
            flux = weno_flux(cells, positive, speed, weight)
            past = jnp.where(lane == 0, pltpu.roll(extra[q], to_high, 1), flux)
            change = pltpu.roll(past, LANES - 1, 1) - flux
            if q == 0:
                pcells = moved(4, tile(A, 4, z), 1, 1)
                change = change + HALF_DT * (pcells[2] - pcells[0])
            acc[q, z] = acc[q, z] - change
            dm[q, z] = cells[3] - cells[2]
            dp[q, z] = cells[4] - cells[3]
        return carry

    lax.fori_loop(0, depth, horizontal, 0)

    for arrive in y_arrive + d_arrive:
        arrive()
    scale = HALF_DT * SMAG_COEF

    def mixing_coefficient(ux, vy, uy, vx):
        cross = uy + vx
        return scale * jnp.sqrt(0.5 * (ux * ux + vy * vy) + (0.25 * (cross * cross) + BACKGROUND))

    def along_y(zt, carry):
        levels = pl.ds(pl.multiple_of(zt * ROWS, ROWS), ROWS)

        def row(q, y):
            if y < 0:
                return YH[0, slot(-1 - y, q), levels]
            if y >= ROWS:
                return YH[1, slot(y - ROWS, q), levels]
            return Af[q, every(zt, y)]

        us = {y: row(0, y) for y in range(-2, ROWS + 2)}
        vs = {y: row(1, y) for y in range(-2, ROWS + 2)}
        eddy = []
        for y in range(-1, ROWS + 1):
            if 0 <= y < ROWS:
                ux, vx = duxf[every(zt, y)], dvxf[every(zt, y)]
            else:
                a = 0 if y < 0 else 1
                both = []
                for q, base in ((0, us[y]), (1, vs[y])):
                    right = pltpu.roll(jnp.where(lane == 0, pltpu.roll(DR[a, 1, 0], lax.rem(LANES - 2 * zt - q, LANES), 1), base), LANES - 1, 1)
                    left = pltpu.roll(jnp.where(lane == LANES - 1, pltpu.roll(DR[a, 0, 0], LANES - 1 - 2 * zt - q, 1), base), 1, 1)
                    both.append(right - left)
                ux, vx = both
            e = mixing_coefficient(ux, vs[y + 1] - vs[y - 1], us[y + 1] - us[y - 1], vx)
            eddy.append(e)
            if 0 <= y < ROWS:
                EAf[every(zt, y)] = e
        speeds, signs, weights, spread = [], [], [], []
        for f in range(ROWS + 1):
            s = HALF_DT * (vs[f - 1] + vs[f])
            speeds.append(s)
            signs.append(s > 0.0)
            weights.append(jnp.abs(s) * (1.0 / 6.0))
            spread.append(eddy[f] + eddy[f + 1])
        for q in range(4):
            cells = [row(q, y) for y in range(-3, ROWS + 3)]
            lower = None
            for f in range(ROWS + 1):
                six = cells[f:f + 6]
                flux = weno_flux(six, signs[f], speeds[f], weights[f]) - spread[f] * (six[3] - six[2])
                if f:
                    y = f - 1
                    value = accf[q, every(zt, y)] - (flux - lower)
                    if q == 1:
                        value = value - HALF_DT * (row(4, y + 1) - row(4, y - 1))
                    if q == 2:
                        value = value + (SECTION_DT * BUOYANCY) * row(3, y)
                    accf[q, every(zt, y)] = value
                lower = flux
        return carry

    lax.fori_loop(0, tiles, along_y, 0)

    def outside(side):
        parts = []
        for q in range(2):
            far, own = RX[side, q], SX[side, q]
            if side == 0:
                plus, base, minus = own, shift(far, 2), shift(far, 1)
                above, below = shift(DR[1, 0, q + 1], 2), shift(DR[0, 0, q + 1], 2)
            else:
                plus, base, minus = shift(far, 1), far, shift(own, 2)
                above, below = DR[1, 1, q + 1], DR[0, 1, q + 1]
            nxt = pltpu.roll(jnp.where(sub == 0, above, base), ROWS - 1, 0)
            prv = pltpu.roll(jnp.where(sub == ROWS - 1, below, base), 1, 0)
            parts.append((plus - minus, nxt - prv))
        (ux, uy), (vx, vy) = parts
        return mixing_coefficient(ux, vy, uy, vx)

    e_low, e_high = outside(0), outside(1)

    for c in stage2:
        c.wait_recv()
    mean = T1[...]
    for k in range(n_gy - 1):
        mean = mean + R2[k]
    mean = mean * (1.0 / (ROWS * LANES * n_gx * n_gy))
    mean = (SECTION_DT * BUOYANCY) * mean
    for zt in range(tiles):
        level = jnp.sum(jnp.where(lane == zt, mean, 0.0), axis=1, keepdims=True)
        MB[zt * ROWS:(zt + 1) * ROWS] = jnp.broadcast_to(level, (ROWS, LANES))

    def final(z, carry):
        e = EA[z]
        low = pltpu.roll(e_low, lax.rem(2 * LANES - 4 * z - 1, LANES), 1)
        high = pltpu.roll(e_high, lax.rem(LANES - 4 * z, LANES), 1)
        before = e + pltpu.roll(jnp.where(lane == LANES - 1, low, e), 1, 1)
        after = e + pltpu.roll(jnp.where(lane == 0, high, e), LANES - 1, 1)
        for q in range(4):
            value = acc[q, z] + (after * dp[q, z] - before * dm[q, z])
            if q == 2:
                value = value - MB[pl.ds(z, 1)]
            out[q, z] = value
        return carry

    lax.fori_loop(0, depth, final, 0, unroll=4)

    for cond, c in moves:
        @pl.when(cond)
        def _():
            c.wait_send()
    for c in stage1 + stage2:
        c.wait_send()


def body(n_gx, n_gy, fields, coriolis, slope_east, slope_north):
    depth = fields.shape[1]
    f32 = jnp.float32
    block = (depth, ROWS, LANES)
    dma = pltpu.SemaphoreType.DMA
    vmem = pl.BlockSpec(memory_space=pltpu.VMEM)
    return pl.pallas_call(
        functools.partial(kernel, n_gx, n_gy, depth),
        out_shape=jax.ShapeDtypeStruct((4,) + block, f32),
        in_specs=[pl.BlockSpec(memory_space=pl.ANY), pl.BlockSpec(memory_space=pltpu.SMEM), vmem, vmem],
        out_specs=vmem,
        scratch_shapes=[
            pltpu.VMEM((5,) + block, f32),
            pltpu.VMEM((4,) + block, f32),
            pltpu.VMEM((4,) + block, f32),
            pltpu.VMEM((4,) + block, f32),
            pltpu.VMEM(block, f32),
            pltpu.VMEM(block, f32),
            pltpu.VMEM(block, f32),
            pltpu.VMEM((2, 5, ROWS, LANES), f32),
            pltpu.VMEM((2, 5, ROWS, LANES), f32),
            pltpu.VMEM((2, 13, depth, LANES), f32),
            pltpu.VMEM((2, 13, depth, LANES), f32),
            pltpu.VMEM((2, 2, 3, ROWS, LANES), f32),
            pltpu.VMEM((2, 2, 3, ROWS, LANES), f32),
            pltpu.VMEM((depth, LANES), f32),
            pltpu.VMEM((ROWS, LANES), f32),
            pltpu.VMEM((ROWS, LANES), f32),
            pltpu.VMEM((n_gx - 1, ROWS, LANES), f32),
            pltpu.VMEM((n_gy - 1, ROWS, LANES), f32),
            dma((5,)),
            dma((2,)), dma((2,)),
            dma((2,)), dma((2,)),
            dma((4,)), dma((4,)),
            dma((n_gx - 1,)), dma((n_gx - 1,)),
            dma((n_gy - 1,)), dma((n_gy - 1,)),
        ],
        compiler_params=pltpu.CompilerParams(collective_id=0, has_side_effects=True),
        name="section",
    )(fields, coriolis, slope_east, slope_north)


def solution(mesh):
    return jax.shard_map(
        functools.partial(body, mesh.shape["gx"], mesh.shape["gy"]),
        mesh=mesh,
        in_specs=(P(None, None, "gx", "gy"), P("gx"), P("gx", "gy"), P("gx", "gy")),
        out_specs=P(None, None, "gx", "gy"),
        check_vma=False,
    )
```
